256 devices in a mesh: row: 16 (over x_hi, z), col: 16 (over x_lo, y, core).
Axes of the slice: x: 4 (x_hi: 2, x_lo: 2; x = x_hi * 2 + x_lo), y: 4, z: 8, core: 2. Of those that a mesh axis runs over, the one named last changes fastest.
Arguments:
- queries: bfloat16 [32768, 768], P(('row', 'col')), may hold values from -6 to 6
- keys: bfloat16 [32768, 768], P(('row', 'col')), may hold values from -6 to 6
- values: bfloat16 [32768, 768], P(('row', 'col')), may hold values from -6 to 6
- query_gain: float32 [128], replicated, may hold values from 0.8 to 3
- key_gain: float32 [128], replicated, may hold values from 0.8 to 3
Outputs:
- attended: bfloat16 [32768, 768], P(('row', 'col'))
The draws below stay inside these ranges and needn't reach their ends.
All inputs are finite; a program needn't handle non-finite values.
Results may differ from the reference program's by a relative error of at most 0.011.
Values may be sent and summed in bfloat16 or wider, within the bound.
No kernel may reach another device: no remote copies, remote signals or barrier semaphores. Data moves between devices by JAX's collectives and lax.ppermute only.
A program may use at most 64 MiB of HBM per device.

```python
import math
import jax
import jax.numpy as jnp
from jax import lax

HEADS = 6
DH = 128
TOKENS = 32768


def block_levels(stream_key, extent, shards, least, high):
    loudness = 1.0
    for position, parts in shards:
        draws = jax.random.uniform(jax.random.fold_in(jax.random.fold_in(stream_key, 6), position), (parts,), jnp.float32, least / len(shards), high / len(shards))
        loudness = loudness * jnp.repeat(jnp.exp(draws), extent[position] // parts).reshape((-1,) + (1,) * (len(extent) - 1 - position))
    return loudness


def normal_values(stream_key, extent, spread, bound, split=(), dtype=jnp.bfloat16):
    level = block_levels(stream_key, extent, split, -0.22, 0.18) if split else 1.0
    array = jax.random.normal(stream_key, extent, jnp.float32) * spread * level
    return jnp.minimum(jnp.maximum(array, -bound), bound).astype(dtype)


def setup_inputs(seed: int = 0) -> dict:
    seeds = jax.random.split(jax.random.key(seed), 6)
    queries = normal_values(seeds[0], (TOKENS, HEADS * DH), 1.0, 6.0, ((0, 256),))
    keys = normal_values(seeds[1], (TOKENS, HEADS * DH), 1.0, 6.0, ((0, 256),))
    values = normal_values(seeds[2], (TOKENS, HEADS * DH), 1.0, 6.0, ((0, 256),))
    query_gain = jnp.clip(jnp.exp(jax.random.uniform(seeds[3], (DH,), jnp.float32, math.log(0.8), math.log(3.0))), 0.8, 3.0)
    key_gain = jnp.clip(jnp.exp(jax.random.uniform(seeds[4], (DH,), jnp.float32, math.log(0.8), math.log(3.0))), 0.8, 3.0)
    return dict(queries=queries, keys=keys, values=values, query_gain=query_gain, key_gain=key_gain)


EPSILON = 0.1

def normed(entries, gain):
    rows = entries.shape[0]
    shaped = entries.reshape(rows, HEADS, DH).astype(jnp.float32)
    inverse = lax.rsqrt(lax.optimization_barrier(jnp.mean(shaped * shaped, axis=-1, keepdims=True)) + EPSILON)
    return (shaped * inverse * gain).astype(jnp.bfloat16).reshape(rows, HEADS * DH)

def reference(queries, keys, values, query_gain, key_gain):
    query_normed = normed(queries, query_gain)
    key_normed = normed(keys, key_gain)
    key_rows = key_normed.reshape(TOKENS, HEADS, DH).astype(jnp.float32)
    value_rows = values.reshape(TOKENS, HEADS, DH).astype(jnp.float32)
    block = math.gcd(TOKENS, 256)
    query_blocks = query_normed.reshape(TOKENS // block, block, HEADS, DH)
    shift = math.log(TOKENS)
    inverse_root = 1.0 / math.sqrt(DH)

    def one_block(query_block):
        scores = jnp.einsum('qhd,khd->hqk', query_block.astype(jnp.float32), key_rows) * inverse_root
        weights = jax.nn.sigmoid(scores - shift).astype(jnp.bfloat16)
        weights = lax.optimization_barrier(weights).astype(jnp.float32)
        mixed = jnp.einsum('hqk,khd->qhd', weights, value_rows)
        return mixed.reshape(block, HEADS * DH)
    attended = lax.map(one_block, query_blocks).reshape(TOKENS, HEADS * DH)
    return attended.astype(jnp.bfloat16)
```

```python
import functools
import math

import jax
import jax.numpy as jnp
from jax import lax
from jax.experimental import pallas as pl
from jax.experimental.pallas import tpu as pltpu
from jax.sharding import Mesh
from jax.sharding import PartitionSpec as P

AXES = ("xh", "z", "xl", "y", "c")
PLANE = ("xh", "xl", "y")
HEADS = 6
DH = 128
HALF = 3
EPSILON = 0.1
SLOPE = -math.log2(math.e) / math.sqrt(DH)

VM = pl.BlockSpec(memory_space=pltpu.VMEM)
SM = pl.BlockSpec(memory_space=pltpu.SMEM)


def prepare_body(half_ref, q_ref, k_ref, v_ref, qg_ref, kg_ref, qt_ref, mine_ref, other_ref, both):
    half = half_ref[0]

    def normed(ref, gain_ref, h):
        x = ref[:, h * DH : (h + 1) * DH].astype(jnp.float32)
        inverse = lax.rsqrt(jnp.mean(x * x, axis=-1, keepdims=True) + EPSILON)
        return x * inverse * gain_ref[...]

    for h in range(HEADS):
        g, i = h // HALF, h % HALF
        both[g, i] = normed(k_ref, kg_ref, h).astype(jnp.bfloat16)
        v = v_ref[:, h * DH : (h + 1) * DH].astype(jnp.float32)
        both[g, HALF + i] = v.T.astype(jnp.bfloat16)
        qt = normed(q_ref, qg_ref, h).T.astype(jnp.bfloat16)
        for d in range(8):
            qt_ref[g * 8 + d, i] = qt
    mine_ref[...] = both[half]
    other_ref[...] = both[1 - half]


def prepare(half, q, k, v, qg, kg):
    rows = q.shape[0]
    pack = jax.ShapeDtypeStruct((2 * HALF, DH, rows), jnp.bfloat16)
    return pl.pallas_call(
        prepare_body,
        out_shape=(jax.ShapeDtypeStruct((16, HALF, DH, rows), jnp.bfloat16), pack, pack),
        in_specs=[SM] + [VM] * 5,
        out_specs=(VM, VM, VM),
        scratch_shapes=[pltpu.VMEM((2, 2 * HALF, DH, rows), jnp.bfloat16)],
        name="prepare",
    )(half, q, k, v, qg, kg)


def attend_body(tokens, kinds, first, last, *refs):
    n = len(kinds)
    qt, out = refs[0], refs[-1]
    total_in = None if first else refs[1 + n]
    units = []
    for ref, pair in zip(refs[1 : 1 + n], kinds):
        units += [ref.at[0], ref.at[1]] if pair else [ref]
    shift = 1.0 / tokens

    def one(i, _):
        for h in range(HALF):
            q = jnp.concatenate([qt[2 * i, h], qt[2 * i + 1, h]], axis=1)
            total = None
            for a, b in zip(units[::2], units[1::2]):
                k = jnp.concatenate([a[h], b[h]], axis=0)
                vt = jnp.concatenate([a[HALF + h], b[HALF + h]], axis=1)
                s = jnp.dot(k, q, preferred_element_type=jnp.float32)
                u = jnp.exp2(s * SLOPE) + shift
                w = jnp.bfloat16(1.0) / u.astype(jnp.bfloat16)
                o = jnp.dot(vt, w, preferred_element_type=jnp.float32)
                total = o if total is None else total + o
            for j in range(2):
                r = total[:, DH * j : DH * (j + 1)]
                if not first:
                    r = r + total_in[2 * i + j, h]
                out[2 * i + j, h] = (r * shift).astype(jnp.bfloat16) if last else r
        return 0

    lax.fori_loop(0, 8, one, 0)


def attend(tokens, qt, blocks, total, last):
    kinds = tuple(b.ndim == 4 for b in blocks)
    first = total is None
    args = [qt, *blocks] + ([] if first else [total])
    keys = 128 * sum(2 if p else 1 for p in kinds)
    pairs = keys * 2048 * HALF
    return pl.pallas_call(
        functools.partial(attend_body, tokens, kinds, first, last),
        out_shape=jax.ShapeDtypeStruct(qt.shape, jnp.bfloat16 if last else jnp.float32),
        in_specs=[VM] * len(args),
        out_specs=VM,
        input_output_aliases={} if first or last else {len(args) - 1: 0},
        cost_estimate=pl.CostEstimate(
            flops=pairs * DH * 4, bytes_accessed=8 << 20, transcendentals=2 * pairs
        ),
        name=f"attend{keys}",
    )(*args)


def finish_body(parts_ref, out_ref):
    for h in range(HEADS):
        g, i = h // HALF, h % HALF
        total = parts_ref[g * 8, i].astype(jnp.float32)
        for s in range(1, 8):
            total = total + parts_ref[g * 8 + s, i].astype(jnp.float32)
        out_ref[:, h * DH : (h + 1) * DH] = total.T.astype(jnp.bfloat16)


def finish(parts, rows):
    return pl.pallas_call(
        finish_body,
        out_shape=jax.ShapeDtypeStruct((rows, HEADS * DH), jnp.bfloat16),
        in_specs=[VM],
        out_specs=VM,
        name="finish",
    )(parts)


def per_device(queries, keys, values, query_gain, key_gain):
    rows = queries.shape[0]
    tokens = rows * lax.axis_size(AXES)
    half = lax.axis_index("xh").astype(jnp.int32).reshape(1)
    qt_send, mine, other = prepare(
        half, queries, keys, values, query_gain.reshape(1, DH), key_gain.reshape(1, DH)
    )
    partner = [(0, 3), (3, 0), (1, 2), (2, 1)]
    n = lax.axis_size("z")
    up = [(i, (i + 1) % n) for i in range(n)]
    down = [(i, (i - 1) % n) for i in range(n)]
    swap = [(0, 1), (1, 0)]

    theirs = lax.ppermute(other, ("xh", "xl"), partner)
    own = lax.all_to_all(qt_send, PLANE, 0, 0, tiled=True)
    block = jnp.stack([mine, theirs])
    groups = [[block]]
    u = d = block
    for step in range(3):
        u, d = lax.ppermute(u, "z", up), lax.ppermute(d, "z", down)
        groups.append([u, d])
    u, d = lax.ppermute(u[0], "z", up), lax.ppermute(d[1], "z", down)
    groups.append([u, d])
    peer = lax.ppermute(own, "c", swap)

    groups = [groups[0] + groups[1], groups[2], groups[3], groups[4]]
    totals = [None, None]
    for s, group in enumerate(groups):
        last = s == len(groups) - 1
        for who in (1, 0):
            totals[who] = attend(tokens, (own, peer)[who], group, totals[who], last)
    back = lax.ppermute(totals[1], "c", swap)
    parts = (totals[0].astype(jnp.float32) + back.astype(jnp.float32)).astype(jnp.bfloat16)
    parts = lax.all_to_all(parts, PLANE, 0, 0, tiled=True)
    return finish(parts, rows)


def solution(mesh):
    torus = Mesh(mesh.devices.reshape(2, 8, 2, 4, 2), AXES)
    return jax.shard_map(
        per_device,
        mesh=torus,
        in_specs=(P(AXES, None), P(AXES, None), P(AXES, None), P(), P()),
        out_specs=P(AXES, None),
        check_vma=False,
    )
```

```python
import functools
import math

import jax
import jax.numpy as jnp
from jax import lax
from jax.experimental import pallas as pl
from jax.experimental.pallas import tpu as pltpu
from jax.sharding import Mesh
from jax.sharding import PartitionSpec as P

AXES = ("xh", "z", "xl", "y", "c")
PLANE = ("xh", "xl", "y")
HEADS = 6
DH = 128
HALF = 3
EPSILON = 0.1
SLOPE = -math.log2(math.e) / math.sqrt(DH)

VM = pl.BlockSpec(memory_space=pltpu.VMEM)
AHEAD = 2
LAG = 2
SM = pl.BlockSpec(memory_space=pltpu.SMEM)


def normed(ref, gain_ref, h):
    x = ref[:, h * DH : (h + 1) * DH].astype(jnp.float32)
    inverse = lax.rsqrt(jnp.mean(x * x, axis=-1, keepdims=True) + EPSILON)
    return x * inverse * gain_ref[...]


def keys_body(half_ref, k_ref, v_ref, kg_ref, mine_ref, other_ref, both):
    half = half_ref[0]
    for h in range(HEADS):
        g, i = h // HALF, h % HALF
        both[g, i] = normed(k_ref, kg_ref, h).astype(jnp.bfloat16)
        v = v_ref[:, h * DH : (h + 1) * DH].astype(jnp.float32)
        both[g, HALF + i] = v.T.astype(jnp.bfloat16)
    mine_ref[...] = both[half]
    other_ref[...] = both[1 - half]


def queries_body(q_ref, qg_ref, after_ref, qt_ref):
    for h in range(HEADS):
        g, i = h // HALF, h % HALF
        qt = normed(q_ref, qg_ref, h).T.astype(jnp.bfloat16)
        for d in range(8):
            qt_ref[g * 8 + d, i] = qt


def prepare_keys(half, k, v, kg):
    rows = k.shape[0]
    pack = jax.ShapeDtypeStruct((2 * HALF, DH, rows), jnp.bfloat16)
    return pl.pallas_call(
        keys_body,
        out_shape=(pack, pack),
        in_specs=[SM] + [VM] * 3,
        out_specs=(VM, VM),
        scratch_shapes=[pltpu.VMEM((2, 2 * HALF, DH, rows), jnp.bfloat16)],
        compiler_params=pltpu.CompilerParams(vmem_limit_bytes=60 << 20),
        name="prepare_keys",
    )(half, k, v, kg)


def prepare_queries(q, qg, after):
    rows = q.shape[0]
    return pl.pallas_call(
        queries_body,
        out_shape=jax.ShapeDtypeStruct((16, HALF, DH, rows), jnp.bfloat16),
        in_specs=[VM, VM, pl.BlockSpec(memory_space=pl.ANY)],
        out_specs=VM,
        compiler_params=pltpu.CompilerParams(vmem_limit_bytes=60 << 20),
        name="prepare_queries",
    )(q, qg, after)


def attend_body(tokens, n, tiles, first, last, *refs):
    qt, out = refs[0], refs[-1]
    units = refs[1 : 1 + n]
    total_in = None if first else refs[1 + n]
    shift = 1.0 / tokens

    pairs = tuple(zip(units[::2], units[1::2]))
    unroll = max(1, tiles // (len(pairs) * HALF))

    def scores(i, h, p):
        a, b = pairs[p]
        q = jnp.concatenate([qt[2 * i, h], qt[2 * i + 1, h]], axis=1)
        k = jnp.concatenate([a[h], b[h]], axis=0)
        return jnp.dot(k, q, preferred_element_type=jnp.float32)

    def weigh(s):
        u = jnp.exp2(s * SLOPE) + shift
        return jnp.bfloat16(1.0) / u.astype(jnp.bfloat16)

    def mixed(h, p, w):
        a, b = pairs[p]
        vt = jnp.concatenate([a[HALF + h], b[HALF + h]], axis=1)
        return jnp.dot(vt, w, preferred_element_type=jnp.float32)

    def store(i, h, total):
        for j in range(2):
            r = total[:, DH * j : DH * (j + 1)]
            if not first:
                r = r + total_in[2 * i + j, h]
            out[2 * i + j, h] = (r * shift).astype(jnp.bfloat16) if last else r

    def group(g, _):
        steps = [
            (g * unroll + t, h, p)
            for t in range(unroll)
            for h in range(HALF)
            for p in range(len(pairs))
        ]
        count = len(steps)
        ahead = [scores(*steps[t]) for t in range(min(AHEAD, count))]
        weights = []
        total = None
        for t in range(count + LAG):
            if t + AHEAD < count:
                ahead.append(scores(*steps[t + AHEAD]))
            if t < count:
                weights.append(weigh(ahead.pop(0)))
            if t >= LAG:
                i, h, p = steps[t - LAG]
                o = mixed(h, p, weights.pop(0))
                total = o if p == 0 else total + o
                if p == len(pairs) - 1:
                    store(i, h, total)
        return 0

    lax.fori_loop(0, 8 // unroll, group, 0)


def attend(tokens, qt, blocks, total, last, tiles=24):
    first = total is None
    args = [qt, *blocks] + ([] if first else [total])
    keys = 128 * len(blocks)
    pairs = keys * 2048 * HALF
    return pl.pallas_call(
        functools.partial(attend_body, tokens, len(blocks), tiles, first, last),
        out_shape=jax.ShapeDtypeStruct(qt.shape, jnp.bfloat16 if last else jnp.float32),
        in_specs=[VM] * len(args),
        out_specs=VM,
        input_output_aliases={} if first or last else {len(args) - 1: 0},
        cost_estimate=pl.CostEstimate(
            flops=pairs * DH * 4, bytes_accessed=8 << 20, transcendentals=2 * pairs
        ),
        compiler_params=pltpu.CompilerParams(vmem_limit_bytes=16 << 20),
    )(*args)


def finish_body(parts_ref, out_ref):
    for h in range(HEADS):
        g, i = h // HALF, h % HALF
        total = parts_ref[g * 8, i].astype(jnp.float32)
        for s in range(1, 8):
            total = total + parts_ref[g * 8 + s, i].astype(jnp.float32)
        out_ref[:, h * DH : (h + 1) * DH] = total.T.astype(jnp.bfloat16)


def finish(parts, rows):
    return pl.pallas_call(
        finish_body,
        out_shape=jax.ShapeDtypeStruct((rows, HEADS * DH), jnp.bfloat16),
        in_specs=[VM],
        out_specs=VM,
        compiler_params=pltpu.CompilerParams(vmem_limit_bytes=8 << 20),
        name="finish",
    )(parts)


def per_device(queries, keys, values, query_gain, key_gain):
    rows = queries.shape[0]
    tokens = rows * lax.axis_size(AXES)
    half = lax.axis_index("xh").astype(jnp.int32).reshape(1)
    mine, other = prepare_keys(half, keys, values, key_gain.reshape(1, DH))
    qt_send = prepare_queries(queries, query_gain.reshape(1, DH), other)
    partner = [(0, 3), (3, 0), (1, 2), (2, 1)]
    n = lax.axis_size("z")
    ring = [(2 * i, 2 * ((i + 1) % n)) for i in range(n)]
    ring += [(2 * i + 1, 2 * ((i - 1) % n) + 1) for i in range(n)]
    swap = [(0, 1), (1, 0)]

    a, b = [mine], []
    b.append(lax.ppermute(other, ("xh", "xl"), partner))
    own = lax.all_to_all(qt_send, PLANE, 0, 0, tiled=True)
    for _ in range(1, n):
        a.append(lax.ppermute(a[-1], ("z", "c"), ring))
        b.append(lax.ppermute(b[-1], ("z", "c"), ring))
    peer = lax.ppermute(own, "c", swap)

    groups = [a[0:4] + b[0:4], a[4:6] + b[4:6], a[6:8] + b[6:8]]
    totals = [None, None]
    for s, group in enumerate(groups):
        last = s == len(groups) - 1
        for who in (1, 0) if last else (0, 1):
            totals[who] = attend(tokens, (own, peer)[who], group, totals[who], last)
    back = lax.ppermute(totals[1], "c", swap)
    parts = (totals[0].astype(jnp.float32) + back.astype(jnp.float32)).astype(jnp.bfloat16)
    parts = lax.all_to_all(parts, PLANE, 0, 0, tiled=True)
    return finish(parts, rows)


def solution(mesh):
    torus = Mesh(mesh.devices.reshape(2, 8, 2, 4, 2), AXES)

    return jax.shard_map(
        per_device,
        mesh=torus,
        in_specs=(P(AXES, None), P(AXES, None), P(AXES, None), P(), P()),
        out_specs=P(AXES, None),
        check_vma=False,
    )
```

```python
import functools
import math

import jax
import jax.numpy as jnp
from jax import lax
from jax.experimental import pallas as pl
from jax.experimental.pallas import tpu as pltpu
from jax.sharding import Mesh
from jax.sharding import PartitionSpec as P

AXES = ("xh", "z", "xl", "y", "c")
PLANE = ("xh", "xl", "y")
HEADS = 6
DH = 128
HALF = 3
EPSILON = 0.1
SLOPE = -math.log2(math.e) / math.sqrt(DH)

VM = pl.BlockSpec(memory_space=pltpu.VMEM)
AHEAD = 2
LAG = 2
RING = ("au1", "ad1", "bu1", "bd1", "au2", "ad2", "bu2", "bd2", "au3", "ad3", "bu3", "bd3", "au4", "bd4")
SM = pl.BlockSpec(memory_space=pltpu.SMEM)


def normed(ref, gain_ref, h):
    x = ref[:, h * DH : (h + 1) * DH].astype(jnp.float32)
    inverse = lax.rsqrt(jnp.mean(x * x, axis=-1, keepdims=True) + EPSILON)
    return x * inverse * gain_ref[...]


def prepare_body(half_ref, q_ref, k_ref, v_ref, qg_ref, kg_ref, qt_ref, mine_ref, other_ref, both):
    half = half_ref[0]
    for h in range(HEADS):
        g, i = h // HALF, h % HALF
        both[g, i] = normed(k_ref, kg_ref, h).astype(jnp.bfloat16)
        v = v_ref[:, h * DH : (h + 1) * DH].astype(jnp.float32)
        both[g, HALF + i] = v.T.astype(jnp.bfloat16)
        qt = normed(q_ref, qg_ref, h).T.astype(jnp.bfloat16)
        for d in range(8):
            qt_ref[g * 8 + d, i] = qt
    mine_ref[...] = both[half]
    other_ref[...] = both[1 - half]


def prepare(half, q, k, v, qg, kg):
    rows = q.shape[0]
    pack = jax.ShapeDtypeStruct((2 * HALF, DH, rows), jnp.bfloat16)
    return pl.pallas_call(
        prepare_body,
        out_shape=(jax.ShapeDtypeStruct((16, HALF, DH, rows), jnp.bfloat16), pack, pack),
        in_specs=[SM] + [VM] * 5,
        out_specs=(VM, VM, VM),
        scratch_shapes=[pltpu.VMEM((2, 2 * HALF, DH, rows), jnp.bfloat16)],
        compiler_params=pltpu.CompilerParams(vmem_limit_bytes=60 << 20),
        name="prepare",
    )(half, q, k, v, qg, kg)


def unroll_of(tiles, each):
    unroll = 8
    while unroll > 1 and unroll * each > tiles:
        unroll //= 2
    return unroll


def attend_body(tokens, n, tiles, first, last, *refs):
    qt, out = refs[0], refs[-1]
    units = refs[1 : 1 + n]
    total_in = None if first else refs[1 + n]
    shift = 1.0 / tokens

    pairs = tuple(zip(units[::2], units[1::2]))
    unroll = unroll_of(tiles, len(pairs) * HALF)

    def scores(i, h, p):
        a, b = pairs[p]
        q = jnp.concatenate([qt[2 * i, h], qt[2 * i + 1, h]], axis=1)
        k = jnp.concatenate([a[h], b[h]], axis=0)
        return jnp.dot(k, q, preferred_element_type=jnp.float32)

    def weigh(s):
        u = jnp.exp2(s * SLOPE) + shift
        return jnp.bfloat16(1.0) / u.astype(jnp.bfloat16)

    def mixed(h, p, w):
        a, b = pairs[p]
        vt = jnp.concatenate([a[HALF + h], b[HALF + h]], axis=1)
        return jnp.dot(vt, w, preferred_element_type=jnp.float32)

    def store(i, h, total):
        for j in range(2):
            r = total[:, DH * j : DH * (j + 1)]
            if not first:
                r = r + total_in[2 * i + j, h]
            out[2 * i + j, h] = (r * shift).astype(jnp.bfloat16) if last else r

    def group(g, _):
        steps = [
            (g * unroll + t, h, p)
            for t in range(unroll)
            for h in range(HALF)
            for p in range(len(pairs))
        ]
        count = len(steps)
        ahead = [scores(*steps[t]) for t in range(min(AHEAD, count))]
        weights = []
        total = None
        for t in range(count + LAG):
            if t + AHEAD < count:
                ahead.append(scores(*steps[t + AHEAD]))
            if t < count:
                weights.append(weigh(ahead.pop(0)))
            if t >= LAG:
                i, h, p = steps[t - LAG]
                o = mixed(h, p, weights.pop(0))
                total = o if p == 0 else total + o
                if p == len(pairs) - 1:
                    store(i, h, total)
        return 0

    lax.fori_loop(0, 8 // unroll, group, 0)


def attend(tokens, qt, blocks, total, last, tiles=72):
    first = total is None
    args = [qt, *blocks] + ([] if first else [total])
    keys = 128 * len(blocks)
    pairs = keys * 2048 * HALF
    return pl.pallas_call(
        functools.partial(attend_body, tokens, len(blocks), tiles, first, last),
        out_shape=jax.ShapeDtypeStruct(qt.shape, jnp.bfloat16 if last else jnp.float32),
        in_specs=[VM] * len(args),
        out_specs=VM,
        input_output_aliases={} if first or last else {len(args) - 1: 0},
        cost_estimate=pl.CostEstimate(
            flops=pairs * DH * 4, bytes_accessed=8 << 20, transcendentals=2 * pairs
        ),
        compiler_params=pltpu.CompilerParams(vmem_limit_bytes=16 << 20),
    )(*args)


def finish_body(parts_ref, out_ref):
    for h in range(HEADS):
        g, i = h // HALF, h % HALF
        total = parts_ref[g * 8, i].astype(jnp.float32)
        for s in range(1, 8):
            total = total + parts_ref[g * 8 + s, i].astype(jnp.float32)
        out_ref[:, h * DH : (h + 1) * DH] = total.T.astype(jnp.bfloat16)


def finish(parts, rows):
    return pl.pallas_call(
        finish_body,
        out_shape=jax.ShapeDtypeStruct((rows, HEADS * DH), jnp.bfloat16),
        in_specs=[VM],
        out_specs=VM,
        compiler_params=pltpu.CompilerParams(vmem_limit_bytes=8 << 20),
        name="finish",
    )(parts)


def per_device(queries, keys, values, query_gain, key_gain):
    rows = queries.shape[0]
    tokens = rows * lax.axis_size(AXES)
    half = lax.axis_index("xh").astype(jnp.int32).reshape(1)
    qt_send, mine, other = prepare(
        half, queries, keys, values, query_gain.reshape(1, DH), key_gain.reshape(1, DH)
    )
    partner = [(0, 3), (3, 0), (1, 2), (2, 1)]
    n = lax.axis_size("z")
    ways = {"u": [(i, (i + 1) % n) for i in range(n)], "d": [(i, (i - 1) % n) for i in range(n)]}
    swap = [(0, 1), (1, 0)]

    theirs = lax.ppermute(other, ("xh", "xl"), partner)
    own = lax.all_to_all(qt_send, PLANE, 0, 0, tiled=True)
    held = {("a", "u", 0): mine, ("a", "d", 0): mine, ("b", "u", 0): theirs, ("b", "d", 0): theirs}
    for name in RING:
        key, way, step = name[0], name[1], int(name[2])
        held[key, way, step] = lax.ppermute(held[key, way, step - 1], "z", ways[way])
    peer = lax.ppermute(own, "c", swap)

    first = [mine, theirs]
    for name in RING[:8]:
        first.append(held[name[0], name[1], int(name[2])])
    second = [held[name[0], name[1], int(name[2])] for name in RING[8:]]
    totals = [None, None]
    for s, group in enumerate((first, second)):
        last = s == 1
        for who in (1, 0) if last else (0, 1):
            totals[who] = attend(tokens, (own, peer)[who], group, totals[who], last)
    back = lax.ppermute(totals[1], "c", swap)
    parts = (totals[0].astype(jnp.float32) + back.astype(jnp.float32)).astype(jnp.bfloat16)
    parts = lax.all_to_all(parts, PLANE, 0, 0, tiled=True)
    return finish(parts, rows)


def solution(mesh):
    torus = Mesh(mesh.devices.reshape(2, 8, 2, 4, 2), AXES)

    return jax.shard_map(
        per_device,
        mesh=torus,
        in_specs=(P(AXES, None), P(AXES, None), P(AXES, None), P(), P()),
        out_specs=P(AXES, None),
        check_vma=False,
    )
```
